32 devices in a mesh: data: 32 (over z, y, x, core).
Axes of the slice: x: 2, y: 2, z: 4, core: 2. Of those that a mesh axis runs over, the one named last changes fastest.
Arguments:
- w_one: float32 [8, 768, 2048], P(None, 'data')
- w_two: float32 [8, 2048, 768], P(None, 'data')
- mom_one: float32 [8, 768, 2048], P(None, 'data')
- mom_two: float32 [8, 2048, 768], P(None, 'data')
- x_zero: bfloat16 [32768, 768], P('data')
- y_zero: bfloat16 [32768, 768], P('data')
- x_one: bfloat16 [32768, 768], P('data')
- y_one: bfloat16 [32768, 768], P('data')
Outputs:
- output 1: float32 [8, 768, 2048], P(None, 'data')
- output 2: float32 [8, 2048, 768], P(None, 'data')
- output 3: float32 [8, 768, 2048], P(None, 'data')
- output 4: float32 [8, 2048, 768], P(None, 'data')
- output 5: float32 [32768], P('data')
- output 6: float32 [32768, 768], P('data')
All inputs are finite; a program needn't handle non-finite values.
Results may differ from the reference program's by a relative error of at most 0.0089424.
Values are sent between devices in bfloat16 or wider.
A program may use at most 1 GiB of HBM per device.

```python
import jax
import jax.numpy as jnp
from jax import lax

DATA_DEVS = 32
TOK_DEV = 1024
LAYERS = 8
D_MODEL = 768
D_FF = 2048

BATCH = DATA_DEVS * TOK_DEV
LEARN_RATE = 0.1
MOMENTUM = 0.9


def draw_rows(key_vals, key_shift, centre, spread):
    base_vals = jax.random.normal(key_vals, (DATA_DEVS, TOK_DEV, D_MODEL), jnp.float32)
    col_shift = jax.random.normal(key_shift, (DATA_DEVS, 1, D_MODEL), jnp.float32)
    return (spread * base_vals + centre + 0.5 * col_shift).reshape(BATCH, D_MODEL).astype(jnp.bfloat16)


def setup_inputs(seed: int = 0) -> dict:
    key_list = jax.random.split(jax.random.key(seed), 16)
    w_one = jax.random.normal(key_list[0], (LAYERS, D_MODEL, D_FF), jnp.float32) * D_MODEL ** -0.5
    w_two = jax.random.normal(key_list[1], (LAYERS, D_FF, D_MODEL), jnp.float32) * (D_FF * LAYERS) ** -0.5
    scale_one = 0.3 * (D_MODEL * D_FF * LAYERS) ** -0.5
    row_one = 1.0 + 0.5 * jax.random.normal(key_list[2], (LAYERS, D_MODEL, 1), jnp.float32)
    col_one = jax.random.normal(key_list[3], (LAYERS, 1, D_FF), jnp.float32)
    mom_one = scale_one * (row_one * col_one + 0.5 * jax.random.normal(key_list[4], (LAYERS, D_MODEL, D_FF), jnp.float32))
    scale_two = 0.3 / D_MODEL
    row_two = 1.0 + 0.5 * jax.random.normal(key_list[5], (LAYERS, D_FF, 1), jnp.float32)
    col_two = jax.random.normal(key_list[6], (LAYERS, 1, D_MODEL), jnp.float32)
    mom_two = scale_two * (row_two * col_two + 0.5 * jax.random.normal(key_list[7], (LAYERS, D_FF, D_MODEL), jnp.float32))
    return {
        "w_one": w_one,
        "w_two": w_two,
        "mom_one": mom_one,
        "mom_two": mom_two,
        "x_zero": draw_rows(key_list[8], key_list[9], 0.6, 0.8),
        "y_zero": draw_rows(key_list[10], key_list[11], -0.5, 0.5),
        "x_one": draw_rows(key_list[12], key_list[13], 0.6, 0.8),
        "y_one": draw_rows(key_list[14], key_list[15], -0.5, 0.5),
    }


def run_stack(w_one_b, w_two_b, h_start):
    def layer_step(h_cur, weights):
        w_in, w_out = weights
        act_in = h_cur.astype(jnp.bfloat16)
        pre_act = jnp.dot(act_in, w_in, preferred_element_type=jnp.float32)
        hidden = jax.nn.gelu(pre_act).astype(jnp.bfloat16)
        h_next = h_cur + jnp.dot(hidden, w_out, preferred_element_type=jnp.float32)
        return h_next, (act_in, pre_act, hidden)
    return lax.scan(layer_step, h_start, (w_one_b, w_two_b))


def local_grads(w_one_b, w_two_b, x_rows, y_rows):
    h_end, saved_vals = run_stack(w_one_b, w_two_b, x_rows.astype(jnp.float32))
    d_start = (h_end - y_rows.astype(jnp.float32)) / (BATCH * D_MODEL)

    def back_step(d_state, layer_vals):
        w_in, w_out, act_in, pre_act, hidden = layer_vals
        d_low = d_state.astype(jnp.bfloat16)
        grad_out = jnp.dot(hidden.T, d_low, preferred_element_type=jnp.float32).astype(jnp.bfloat16)
        d_hidden = jnp.dot(d_low, w_out.T, preferred_element_type=jnp.float32)
        d_pre = jax.vjp(jax.nn.gelu, pre_act)[1](d_hidden)[0].astype(jnp.bfloat16)
        grad_in = jnp.dot(act_in.T, d_pre, preferred_element_type=jnp.float32).astype(jnp.bfloat16)
        d_next = d_state + jnp.dot(d_pre, w_in.T, preferred_element_type=jnp.float32)
        return d_next, (grad_in, grad_out)

    act_ins, pre_acts, hiddens = saved_vals
    return lax.scan(back_step, d_start, (w_one_b, w_two_b, act_ins, pre_acts, hiddens), reverse=True)[1]


def reference(w_one, w_two, mom_one, mom_two, x_zero, y_zero, x_one, y_one):
    w_one_b = w_one.astype(jnp.bfloat16)
    w_two_b = w_two.astype(jnp.bfloat16)
    x_dev = x_zero.reshape(DATA_DEVS, TOK_DEV, D_MODEL)
    y_dev = y_zero.reshape(DATA_DEVS, TOK_DEV, D_MODEL)

    def add_device(acc_pair, row_pair):
        grad_in, grad_out = local_grads(w_one_b, w_two_b, row_pair[0], row_pair[1])
        return (acc_pair[0] + grad_in.astype(jnp.float32), acc_pair[1] + grad_out.astype(jnp.float32)), None

    zeros_pair = (jnp.zeros(w_one.shape, jnp.float32), jnp.zeros(w_two.shape, jnp.float32))
    grad_sums = lax.scan(add_device, zeros_pair, (x_dev, y_dev))[0]
    new_mom_one = MOMENTUM * mom_one + grad_sums[0].astype(jnp.bfloat16).astype(jnp.float32)
    new_mom_two = MOMENTUM * mom_two + grad_sums[1].astype(jnp.bfloat16).astype(jnp.float32)
    new_w_one = w_one - LEARN_RATE * new_mom_one
    new_w_two = w_two - LEARN_RATE * new_mom_two
    next_one_b = new_w_one.astype(jnp.bfloat16)
    next_two_b = new_w_two.astype(jnp.bfloat16)

    def device_forward(x_rows):
        return run_stack(next_one_b, next_two_b, x_rows.astype(jnp.float32))[0]

    h_last = lax.map(device_forward, x_one.reshape(DATA_DEVS, TOK_DEV, D_MODEL)).reshape(BATCH, D_MODEL)
    loss_rows = jnp.sum(jnp.square(h_last - y_one.astype(jnp.float32)), axis=1) / (2 * D_MODEL)
    return new_w_one, new_w_two, new_mom_one, new_mom_two, loss_rows, h_last
```

```python
import functools
import math

import jax
import jax.numpy as jnp
from jax import lax
from jax.experimental import pallas as pl
from jax.experimental.pallas import tpu as pltpu
from jax.sharding import PartitionSpec as P

LEARN_RATE = 0.1
MOMENTUM = 0.9
MESH = pl.DeviceIdType.MESH
F32 = jnp.float32
BF16 = jnp.bfloat16
TILE = 256
VMEM_BYTES = 67_000_000
GELU_K = math.sqrt(2.0 / math.pi)
GELU_C = 0.044715


def place():
    me = lax.axis_index("data")
    return lax.div(me, 8), lax.rem(lax.div(me, 4), 2), lax.rem(lax.div(me, 2), 2), lax.rem(me, 2)


def index_of(z, y, x, c):
    return ((z * 2 + y) * 2 + x) * 2 + c


def ring_z(z, step):
    return lax.rem(z + step + 4, 4)


def greet(z, y, x, c):
    barrier = pltpu.get_barrier_semaphore()
    peers = [index_of(ring_z(z, k), y, x, c) for k in (1, 2, 3)]
    peers += [index_of(z, y, 1 - x, c), index_of(z, 1 - y, x, c), index_of(z, y, x, 1 - c)]
    for peer in peers:
        pl.semaphore_signal(barrier, inc=1, device_id=(peer,), device_id_type=MESH)
    pl.semaphore_wait(barrier, len(peers))


def remote(src, dst, send_sem, recv_sem, peer):
    return pltpu.make_async_remote_copy(
        src_ref=src, dst_ref=dst, send_sem=send_sem, recv_sem=recv_sem, device_id=(peer,), device_id_type=MESH
    )


def dot(a, b):
    return jnp.dot(a, b, preferred_element_type=F32)


def dot_t(a, b):
    return lax.dot_general(a, b, (((1,), (1,)), ((), ())), preferred_element_type=F32)


def whole(blocks):
    w = blocks[...]
    return w.reshape(math.prod(w.shape[:-1]), w.shape[-1])


def gelu(u):
    return (0.5 * u) * (1.0 + jnp.tanh(GELU_K * (u + GELU_C * (u * u * u))))


def forward_kernel(save, *refs):
    w1s, w2s, x_in, g1, g2, h = refs[:6]
    refs = refs[6:]
    if save:
        u_out, at_out, zt_out = refs[:3]
        refs = refs[3:]
    w1v, w2v, own_sem, load_sem, send_sem, recv_sem = refs[:6]
    if save:
        u_v, at_v, zt_v, save_sem = refs[6:]
    layers = w1s.shape[0]
    z, y, x, c = place()
    shard, full = (w1s, w2s), (g1, g2)
    tiles = x_in.shape[0] // TILE

    greet(z, y, x, c)

    def z_copy(t, l, k, from_z):
        return remote(
            shard[t].at[l], full[t].at[l, from_z, y, x, c], send_sem.at[t, l, k - 1], recv_sem.at[t, l, k - 1],
            index_of(ring_z(z, k), y, x, c),
        )

    def hop(t, s, l, arriving):
        g = full[t].at[l]
        along_x = (t == 0) == (s == 0)
        if s == 2:
            region = g.at[:, :, :, 1 - c if arriving else c]
            peer = index_of(z, y, x, 1 - c)
        else:
            xs = 1 - x if arriving and along_x else x
            ys = 1 - y if arriving and not along_x else y
            if s == 0:
                region = g.at[:, ys, xs, c]
            elif along_x:
                region = g.at[:, :, xs, c]
            else:
                region = g.at[:, ys, :, c]
            peer = index_of(z, y, 1 - x, c) if along_x else index_of(z, 1 - y, x, c)
        return remote(region, region, send_sem.at[t, l, 3 + s], recv_sem.at[t, l, 3 + s], peer)

    own = [pltpu.make_async_copy(shard[t], full[t].at[:, z, y, x, c], own_sem.at[t]) for t in (0, 1)]
    for copy in own:
        copy.start()

    def send_z(l, carry):
        for t in (0, 1):
            for k in (1, 2, 3):
                z_copy(t, l, k, z).start()
        return carry

    lax.fori_loop(0, layers, send_z, 0)
    h[...] = x_in[...].astype(F32)
    for copy in own:
        copy.wait()

    def u_save(l, rows, m):
        return pltpu.make_async_copy(u_v.at[rows], u_out.at[l, rows], save_sem.at[m])

    def at_save(l):
        return pltpu.make_async_copy(at_v, at_out.at[l], save_sem.at[tiles])

    def zt_save(l):
        return pltpu.make_async_copy(zt_v, zt_out.at[l], save_sem.at[tiles + 1])

    def compute(l):
        load1 = pltpu.make_async_copy(g1.at[l], w1v, load_sem.at[0])
        load2 = pltpu.make_async_copy(g2.at[l], w2v, load_sem.at[1])
        load1.start()
        load2.start()
        if save:
            @pl.when(l > 0)
            def _():
                at_save(l - 1).wait()
                zt_save(l - 1).wait()
        load1.wait()
        load2.wait()

        def tile(m, carry):
            start = pl.multiple_of(m * TILE, TILE)
            rows = pl.ds(start, TILE)
            a = h[rows, :].astype(BF16)
            u = dot(a, whole(w1v))
            act = gelu(u).astype(BF16)
            if save:
                @pl.when(l > 0)
                def _():
                    u_save(l - 1, rows, m).wait()
                u_v[rows, :] = u
                u_save(l, rows, m).start()
                at_v[:, rows] = a.T
                zt_v[:, rows] = act.T
            h[rows, :] += dot(act, whole(w2v))
            return carry

        lax.fori_loop(0, tiles, tile, 0)
        if save:
            at_save(l).start()
            zt_save(l).start()

    def step(it, carry):
        l = it - 3

        @pl.when(l + 3 < layers)
        def _():
            for t in (0, 1):
                for k in (1, 2, 3):
                    z_copy(t, l + 3, k, ring_z(z, -k)).wait_recv()
                hop(t, 0, l + 3, False).start()

        @pl.when((l + 2 >= 0) & (l + 2 < layers))
        def _():
            for t in (0, 1):
                hop(t, 0, l + 2, True).wait_recv()
                hop(t, 1, l + 2, False).start()

        @pl.when(l >= 0)
        def _():
            for t in (0, 1):
                hop(t, 2, l, True).wait_recv()
            compute(l)

        @pl.when((l + 1 >= 0) & (l + 1 < layers))
        def _():
            for t in (0, 1):
                hop(t, 1, l + 1, True).wait_recv()
                hop(t, 2, l + 1, False).start()

        return carry

    lax.fori_loop(0, layers + 3, step, 0)

    def drain(l, carry):
        for t in (0, 1):
            for k in (1, 2, 3):
                z_copy(t, l, k, z).wait_send()
            for s in (0, 1, 2):
                hop(t, s, l, False).wait_send()
        return carry

    lax.fori_loop(0, layers, drain, 0)
    if save:
        for m in range(tiles):
            u_save(layers - 1, pl.ds(m * TILE, TILE), m).wait()
        at_save(layers - 1).wait()
        zt_save(layers - 1).wait()


def forward(save, ident, w1s, w2s, x_in):
    layers, r1, d_ff = w1s.shape
    r2 = w2s.shape[1]
    tok, d_model = x_in.shape
    tiles = tok // TILE
    sds = jax.ShapeDtypeStruct
    hbm, vmem = pl.BlockSpec(memory_space=pl.ANY), pl.BlockSpec(memory_space=pltpu.VMEM)
    outs = [sds((layers, 4, 2, 2, 2, r1, d_ff), BF16), sds((layers, 4, 2, 2, 2, r2, d_model), BF16), sds((tok, d_model), F32)]
    out_specs = [hbm, hbm, vmem]
    scratch = [
        pltpu.VMEM((4, 2, 2, 2, r1, d_ff), BF16),
        pltpu.VMEM((4, 2, 2, 2, r2, d_model), BF16),
        pltpu.SemaphoreType.DMA((2,)),
        pltpu.SemaphoreType.DMA((2,)),
        pltpu.SemaphoreType.DMA((2, layers, 6)),
        pltpu.SemaphoreType.DMA((2, layers, 6)),
    ]
    if save:
        outs += [sds((layers, tok, d_ff), F32), sds((layers, d_model, tok), BF16), sds((layers, d_ff, tok), BF16)]
        out_specs += [hbm, hbm, hbm]
        scratch += [
            pltpu.VMEM((tok, d_ff), F32),
            pltpu.VMEM((d_model, tok), BF16),
            pltpu.VMEM((d_ff, tok), BF16),
            pltpu.SemaphoreType.DMA((tiles + 2,)),
        ]
    return pl.pallas_call(
        functools.partial(forward_kernel, save),
        out_shape=outs,
        in_specs=[vmem, vmem, vmem],
        out_specs=out_specs,
        scratch_shapes=scratch,
        compiler_params=pltpu.CompilerParams(collective_id=ident, has_side_effects=True, vmem_limit_bytes=VMEM_BYTES),
        name="forward_save" if save else "forward_last",
    )(w1s, w2s, x_in)


def gelu_back(u, q):
    t = jnp.tanh(GELU_K * (u + GELU_C * (u * u * u)))
    slope = 0.5 * (1.0 + t) + (0.5 * GELU_K) * u * (1.0 - t * t) * (1.0 + (3.0 * GELU_C) * (u * u))
    return slope * q


def backward_kernel(*refs):
    g1, g2, u_in, at_in, zt_in, d_in, s1, s2, d, d_low, w1v, w2v, u_v, at_v, zt_v, r_v = refs[:16]
    bufs = (refs[16:24], refs[24:32])
    load_sem, send_sem, recv_sem, free_sem = refs[32:]
    sums = (s1, s2)
    layers = s1.shape[0]
    z, y, x, c = place()
    tok = d.shape[0]
    tiles = tok // TILE

    greet(z, y, x, c)

    x_peer, y_peer, core_peer = index_of(z, y, 1 - x, c), index_of(z, 1 - y, x, c), index_of(z, y, x, 1 - c)

    def peer_of(t, s):
        if s == 0:
            return core_peer
        return y_peer if (t == 0) == (s == 1) else x_peer

    def exchange(t, s):
        grad, got0, part, got1, quart, got2, line, got3 = bufs[t]
        if s == 0:
            src, dst = grad.at[:, :, :, 1 - c], got0
        elif s == 1:
            src, dst = (part.at[:, 1 - y] if t == 0 else part.at[:, :, 1 - x]), got1
        else:
            src, dst = quart.at[:, 1 - x if t == 0 else 1 - y], got2
        return remote(src, dst, send_sem.at[t, s], recv_sem.at[t, s], peer_of(t, s))

    def line_send(t, k):
        line, got3 = bufs[t][6], bufs[t][7]
        to = ring_z(z, k)
        return remote(line.at[to], got3.at[k - 1], send_sem.at[t, 2 + k], recv_sem.at[t, 2 + k], index_of(to, y, x, c))

    def give(l, sem, peer):
        @pl.when(l > 0)
        def _():
            pl.semaphore_signal(sem, inc=1, device_id=(peer,), device_id_type=MESH)

    def take(l, sem):
        @pl.when(l < layers - 1)
        def _():
            pl.semaphore_wait(sem, 1)

    def send(t, s, l):
        take(l, free_sem.at[t, s])
        exchange(t, s).start()

    def add(a, b):
        return (a.astype(F32) + b.astype(F32)).astype(BF16)

    def finish(t, l):
        line, got3 = bufs[t][6], bufs[t][7]
        for k in (1, 2, 3):
            line_send(t, k).wait_recv()
        total = line[z].astype(F32) + got3[0].astype(F32) + got3[1].astype(F32) + got3[2].astype(F32)
        sums[t][l] = total.astype(BF16)
        for k in (1, 2, 3):
            line_send(t, k).wait_send()
            give(l, free_sem.at[t, 2 + k], index_of(ring_z(z, -k), y, x, c))

    def to_line(t, l):
        quart, got2, line = bufs[t][4:7]
        exchange(t, 2).wait_recv()
        mine = x if t == 0 else y
        for zz in range(4):
            line[zz] = add(quart[zz, mine], got2[zz])
        exchange(t, 2).wait_send()
        give(l, free_sem.at[t, 2], peer_of(t, 2))
        for k in (1, 2, 3):
            take(l, free_sem.at[t, 2 + k])
            line_send(t, k).start()

    def to_quart(t, l):
        part, got1, quart = bufs[t][2:5]
        exchange(t, 1).wait_recv()

        def body(zz, carry):
            for j in (0, 1):
                own = part[zz, y, j] if t == 0 else part[zz, j, x]
                quart[zz, j] = add(own, got1[zz, j])
            return carry

        lax.fori_loop(0, 4, body, 0)
        exchange(t, 1).wait_send()
        give(l, free_sem.at[t, 1], peer_of(t, 1))
        send(t, 2, l)

    def to_part(t, l):
        grad, got0, part = bufs[t][:3]
        exchange(t, 0).wait_recv()

        def body(zz, carry):
            for yy in (0, 1):
                for xx in (0, 1):
                    part[zz, yy, xx] = add(grad[zz, yy, xx, c], got0[zz, yy, xx])
            return carry

        lax.fori_loop(0, 4, body, 0)
        exchange(t, 0).wait_send()
        give(l, free_sem.at[t, 0], peer_of(t, 0))
        send(t, 1, l)

    loads = (
        (lambda l: g1.at[l], w1v),
        (lambda l: g2.at[l], w2v),
        (lambda l: u_in.at[l], u_v),
        (lambda l: at_in.at[l], at_v),
        (lambda l: zt_in.at[l], zt_v),
    )

    def load(n, l):
        return pltpu.make_async_copy(loads[n][0](l), loads[n][1], load_sem.at[n])

    def prefetch(n, l):
        @pl.when(l > 0)
        def _():
            load(n, l - 1).start()

    def put(t, zz, res):
        grad = bufs[t][0]
        rows = grad.shape[4]
        for k in range(8):
            grad[zz, k // 4, k // 2 % 2, k % 2] = res[k * rows:(k + 1) * rows].astype(BF16)

    def compute(l):
        d_low[...] = d[...].astype(BF16)
        load(4, l).wait()

        def grad_two(zz, carry):
            step = d_two // 4
            put(1, zz, dot(zt_v[pl.ds(pl.multiple_of(zz * step, step), step), :], d_low[...]))
            return carry

        d_two = zt_v.shape[0]
        lax.fori_loop(0, 4, grad_two, 0)
        send(1, 0, l)
        prefetch(4, l)
        load(1, l).wait()
        load(2, l).wait()

        def pre(m, carry):
            rows = pl.ds(pl.multiple_of(m * TILE, TILE), TILE)
            q = dot_t(d_low[rows, :], whole(w2v))
            r_v[rows, :] = gelu_back(u_v[rows, :], q).astype(BF16)
            return carry

        lax.fori_loop(0, tiles, pre, 0)
        prefetch(1, l)
        prefetch(2, l)
        load(3, l).wait()

        def grad_one(zz, carry):
            step = at_v.shape[0] // 4
            put(0, zz, dot(at_v[pl.ds(pl.multiple_of(zz * step, step), step), :], r_v[...]))
            return carry

        lax.fori_loop(0, 4, grad_one, 0)
        send(0, 0, l)
        prefetch(3, l)
        load(0, l).wait()

        @pl.when(l > 0)
        def _():
            def back(m, carry):
                rows = pl.ds(pl.multiple_of(m * TILE, TILE), TILE)
                d[rows, :] += dot_t(r_v[rows, :], whole(w1v))
                return carry

            lax.fori_loop(0, tiles, back, 0)

        prefetch(0, l)

    first = pltpu.make_async_copy(d_in, d, load_sem.at[len(loads)])
    first.start()
    for n in range(len(loads)):
        load(n, layers - 1).start()
    first.wait()

    def step(it, carry):
        l = layers - 1 - it
        for lag, stage in ((4, finish), (3, to_line), (2, to_quart), (1, to_part)):
            @pl.when((l + lag >= 0) & (l + lag < layers))
            def _():
                for t in (1, 0):
                    stage(t, l + lag)

        @pl.when(l >= 0)
        def _():
            compute(l)

        return carry

    lax.fori_loop(0, layers + 4, step, 0)


def backward(ident, g1, g2, u_all, at_all, zt_all, d_state):
    layers, r1, d_ff = g1.shape[0], g1.shape[5], g1.shape[6]
    r2 = g2.shape[5]
    tok, d_model = d_state.shape
    sds = jax.ShapeDtypeStruct
    hbm, vmem = pl.BlockSpec(memory_space=pl.ANY), pl.BlockSpec(memory_space=pltpu.VMEM)
    scratch = [
        pltpu.VMEM((tok, d_model), F32),
        pltpu.VMEM((tok, d_model), BF16),
        pltpu.VMEM((4, 2, 2, 2, r1, d_ff), BF16),
        pltpu.VMEM((4, 2, 2, 2, r2, d_model), BF16),
        pltpu.VMEM((tok, d_ff), F32),
        pltpu.VMEM((d_model, tok), BF16),
        pltpu.VMEM((d_ff, tok), BF16),
        pltpu.VMEM((tok, d_ff), BF16),
    ]
    for block in ((r1, d_ff), (r2, d_model)):
        for lead in ((4, 2, 2, 2), (4, 2, 2), (4, 2, 2), (4, 2), (4, 2), (4,), (4,), (3,)):
            scratch.append(pltpu.VMEM(lead + block, BF16))
    scratch += [
        pltpu.SemaphoreType.DMA((6,)),
        pltpu.SemaphoreType.DMA((2, 6)),
        pltpu.SemaphoreType.DMA((2, 6)),
        pltpu.SemaphoreType.REGULAR((2, 6)),
    ]
    return pl.pallas_call(
        backward_kernel,
        out_shape=[sds((layers, r1, d_ff), BF16), sds((layers, r2, d_model), BF16)],
        in_specs=[hbm] * 6,
        out_specs=[vmem, vmem],
        scratch_shapes=scratch,
        compiler_params=pltpu.CompilerParams(collective_id=ident, has_side_effects=True, vmem_limit_bytes=VMEM_BYTES),
        name="backward",
    )(g1, g2, u_all, at_all, zt_all, d_state)


def solution(mesh):
    n_dev = mesh.shape["data"]
    w_spec = P(None, "data", None)
    row_spec = P("data", None)

    def device_step(w_one, w_two, mom_one, mom_two, x_zero, y_zero, x_one, y_one):
        tok_dev, d_model = x_zero.shape
        g1, g2, h_end, u_all, at_all, zt_all = forward(True, 0, w_one.astype(BF16), w_two.astype(BF16), x_zero)
        d_state = (h_end - y_zero.astype(F32)) / (n_dev * tok_dev * d_model)
        sum_one, sum_two = backward(1, g1, g2, u_all, at_all, zt_all, d_state)
        new_mom_one = MOMENTUM * mom_one + sum_one.astype(F32)
        new_mom_two = MOMENTUM * mom_two + sum_two.astype(F32)
        new_w_one = w_one - LEARN_RATE * new_mom_one
        new_w_two = w_two - LEARN_RATE * new_mom_two
        h_last = forward(False, 2, new_w_one.astype(BF16), new_w_two.astype(BF16), x_one)[2]
        loss_rows = jnp.sum(jnp.square(h_last - y_one.astype(F32)), axis=1) / (2 * d_model)
        return new_w_one, new_w_two, new_mom_one, new_mom_two, loss_rows, h_last

    return jax.shard_map(device_step, mesh=mesh, in_specs=(w_spec, w_spec, w_spec, w_spec, row_spec, row_spec, row_spec, row_spec), out_specs=(w_spec, w_spec, w_spec, w_spec, P("data"), row_spec), check_vma=False)
```

```python
import functools
import math

import jax
import jax.numpy as jnp
from jax import lax
from jax.experimental import pallas as pl
from jax.experimental.pallas import tpu as pltpu
from jax.sharding import PartitionSpec as P

LEARN_RATE = 0.1
MOMENTUM = 0.9
MESH = pl.DeviceIdType.MESH
F32 = jnp.float32
BF16 = jnp.bfloat16
TILE = 256
AHEAD = 5
LINE_AT = 0
VMEM_BYTES = 67_000_000
GELU_K = math.sqrt(2.0 / math.pi)
GELU_C = 0.044715


def place():
    me = lax.axis_index("data")
    return lax.div(me, 8), lax.rem(lax.div(me, 4), 2), lax.rem(lax.div(me, 2), 2), lax.rem(me, 2)


def index_of(z, y, x, c):
    return ((z * 2 + y) * 2 + x) * 2 + c


def ring_z(z, step):
    return lax.rem(z + step + 4, 4)


def greet(z, y, x, c):
    barrier = pltpu.get_barrier_semaphore()
    peers = [index_of(ring_z(z, k), y, x, c) for k in (1, 2, 3)]
    peers += [index_of(z, y, 1 - x, c), index_of(z, 1 - y, x, c), index_of(z, y, x, 1 - c)]
    for peer in peers:
        pl.semaphore_signal(barrier, inc=1, device_id=(peer,), device_id_type=MESH)
    pl.semaphore_wait(barrier, len(peers))


def remote(src, dst, send_sem, recv_sem, peer):
    return pltpu.make_async_remote_copy(
        src_ref=src, dst_ref=dst, send_sem=send_sem, recv_sem=recv_sem, device_id=(peer,), device_id_type=MESH
    )


def dot(a, b):
    return jnp.dot(a, b, preferred_element_type=F32)


def dot_t(a, b):
    return lax.dot_general(a, b, (((1,), (1,)), ((), ())), preferred_element_type=F32)


def whole(blocks):
    w = blocks[...]
    return w.reshape(math.prod(w.shape[:-1]), w.shape[-1])


def gelu(u):
    return (0.5 * u) * (1.0 + jnp.tanh(GELU_K * (u + GELU_C * (u * u * u))))


def forward_kernel(save, scale, *refs):
    w1f, w2f, x_in, y_in = refs[:4] if save else refs[:3] + (None,)
    g1, g2, h = refs[4:7] if save else refs[3:6]
    refs = refs[7:] if save else refs[6:]
    if save:
        u_out, at_out, zt_out = refs[:3]
        refs = refs[3:]
    w1s, w2s = refs[:2]
    refs = refs[2:]
    far = 6 if save else 5
    w1v, w2v, own_sem, load_sem, send_sem, recv_sem, line_sems = refs[:7]
    if save:
        u_v, at_v, zt_v, save_sem = refs[7:]
    layers = w1s.shape[0]
    z, y, x, c = place()
    shard, full = (w1s, w2s), (g1, g2)
    tiles = x_in.shape[0] // TILE
    w1s[...] = w1f[...].astype(BF16)
    w2s[...] = w2f[...].astype(BF16)

    greet(z, y, x, c)

    def z_copy(t, l, k, from_z):
        return remote(
            shard[t].at[l], full[t].at[l, from_z, y, x, c], send_sem.at[t, k - 1], recv_sem.at[t, l, k - 1],
            index_of(ring_z(z, k), y, x, c),
        )

    def half(t, l, other, core):
        g = full[t].at[l]
        if t == 0:
            return g.at[:, 1 - y if other else y, :, core]
        return g.at[:, :, 1 - x if other else x, core]

    def hop(t, s, l, arriving):
        if s == 1:
            region = half(t, l, arriving, c)
            peer = index_of(z, 1 - y, x, c) if t == 0 else index_of(z, y, 1 - x, c)
        else:
            region = half(t, l, s == 3, 1 - c if arriving else c)
            peer = index_of(z, y, x, 1 - c)
        return remote(region, region, send_sem.at[t, 3 + s], recv_sem.at[t, l, 3 + s], peer)

    def first(t, l, k):
        region = full[t].at[l, ring_z(z, -k), y, x, c]
        src = region if k else shard[t].at[l]
        peer = index_of(z, y, 1 - x, c) if t == 0 else index_of(z, 1 - y, x, c)
        return remote(src, region, send_sem.at[t, 3], recv_sem.at[t, l, 3 if k else 7], peer)

    def first_arrived(t, l):
        first(t, l, 0).wait_recv()
        region = full[t].at[l, 0:3, y, x, c]
        remote(region, region, send_sem.at[t, 3], recv_sem.at[t, l, 3], index_of(z, y, x, 1 - c)).wait_recv()

    def plane(p, t, arriving):
        along_x = (t == 0) == (p == 0)
        xs = 1 - x if arriving and along_x else x
        ys = 1 - y if arriving and not along_x else y
        g = full[t].at[far, z]
        if p == 0:
            region = g.at[ys, xs, c]
        else:
            region = g.at[:, xs, c] if along_x else g.at[ys, :, c]
        src = region if p or arriving else shard[t].at[far]
        peer = index_of(z, y, 1 - x, c) if along_x else index_of(z, 1 - y, x, c)
        return remote(src, region, send_sem.at[t, 7 + p], recv_sem.at[t, far, p], peer)

    def line(j, t, way, arriving):
        region = full[t].at[far, z - way * (j if arriving else j - 1), :, :, c]
        n = 2 * j - 2 + (way > 0)
        return remote(region, region, line_sems.at[0, t, n], line_sems.at[1, t, n], index_of(z + way, y, x, c))

    def skip_far(n):
        return jnp.where(n < far, n, n + 1)

    def within(zz):
        return (zz >= 0) & (zz < 4)

    def line_step(j):
        for t in (0, 1):
            for way in (1, -1):
                if j > 1:
                    @pl.when(within(z - way * (j - 1)))
                    def _():
                        line(j - 1, t, way, True).wait_recv()
                if j < 4:
                    @pl.when(within(z - way * (j - 1)) & within(z + way))
                    def _():
                        line(j, t, way, False).start()

    def send_z(l, carry):
        @pl.when(l != far)
        def _():
            for t in (0, 1):
                for k in (1, 2, 3):
                    z_copy(t, l, k, z).start()
        return carry

    def send_own(l, carry):
        @pl.when(l != far)
        def _():
            for t in (0, 1):
                first(t, l, 0).start()
        return carry

    def z_to_first(t, l):
        for k in (1, 2, 3):
            z_copy(t, l, k, ring_z(z, -k)).wait_recv()
            first(t, l, k).start()

    def to_plane(t, l):
        first_arrived(t, l)
        hop(t, 1, l, False).start()
        hop(t, 2, l, False).start()

    def to_core(t, l):
        hop(t, 1, l, True).wait_recv()
        hop(t, 3, l, False).start()

    own = [pltpu.make_async_copy(shard[t], full[t].at[:, z, y, x, c], own_sem.at[t]) for t in (0, 1)]
    for t in (0, 1):
        plane(0, t, False).start()
    lax.fori_loop(0, AHEAD, send_z, 0)
    lax.fori_loop(0, layers, send_own, 0)
    for copy in own:
        copy.start()
    h[...] = x_in[...].astype(F32)
    for t in (0, 1):
        own[t].wait()
        plane(0, t, True).wait_recv()
        plane(1, t, False).start()

    def u_save(l, rows, m):
        return pltpu.make_async_copy(u_v.at[rows], u_out.at[l, rows], save_sem.at[m])

    def at_save(l):
        return pltpu.make_async_copy(at_v, at_out.at[l], save_sem.at[tiles])

    def zt_save(l):
        return pltpu.make_async_copy(zt_v, zt_out.at[l], save_sem.at[tiles + 1])

    def compute(l):
        load1 = pltpu.make_async_copy(g1.at[l], w1v, load_sem.at[0])
        load2 = pltpu.make_async_copy(g2.at[l], w2v, load_sem.at[1])
        load1.start()
        load2.start()
        if save:
            @pl.when(l > 0)
            def _():
                at_save(l - 1).wait()
                zt_save(l - 1).wait()
        load1.wait()
        load2.wait()

        def tile(m, carry):
            start = pl.multiple_of(m * TILE, TILE)
            rows = pl.ds(start, TILE)
            a = h[rows, :].astype(BF16)
            u = dot(a, whole(w1v))
            act = gelu(u).astype(BF16)
            if save:
                @pl.when(l > 0)
                def _():
                    u_save(l - 1, rows, m).wait()
                u_v[rows, :] = u
                u_save(l, rows, m).start()
                at_v[:, rows] = a.T
                zt_v[:, rows] = act.T
            h[rows, :] += dot(act, whole(w2v))
            return carry

        lax.fori_loop(0, tiles, tile, 0)
        if save:
            at_save(l).start()
            zt_save(l).start()

    for stage in (z_to_first, to_plane):
        for t in (0, 1):
            stage(t, 0)
    for l in (1, 2):
        for t in (0, 1):
            z_to_first(t, l)
    for t in (0, 1):
        to_plane(t, 1)
    for t in (0, 1):
        to_core(t, 0)

    def step(l, carry):
        @pl.when(l + AHEAD < layers)
        def _():
            send_z(l + AHEAD, 0)

        third, second = skip_far(l + 3), skip_far(l + 2)

        @pl.when(third < layers)
        def _():
            for t in (0, 1):
                z_to_first(t, third)

        @pl.when(second < layers)
        def _():
            for t in (0, 1):
                to_plane(t, second)

        for j in (1, 2, 3, 4):
            @pl.when(l == LINE_AT + j)
            def _():
                if j == 1:
                    for t in (0, 1):
                        plane(1, t, True).wait_recv()
                line_step(j)

        for t in (0, 1):
            hop(t, 2, l, True).wait_recv()
            hop(t, 3, l, True).wait_recv()
        compute(l)

        @pl.when(l + 1 < layers)
        def _():
            for t in (0, 1):
                @pl.when(l + 1 != far)
                def _():
                    to_core(t, l + 1)

                @pl.when(l + 1 == far)
                def _():
                    hop(t, 2, far, False).start()
                    hop(t, 3, far, False).start()

        return carry

    lax.fori_loop(0, layers, step, 0)

    others = pl.ds(0, layers - 1)
    for t in (0, 1):
        f = full[t]
        sent = [f.at[others, z, y, x, c]] * 3
        sent += [f.at[others, :, y, x, c], f.at[others, :, y, :, c] if t == 0 else f.at[others, :, :, x, c]]
        sent += [f.at[:, :, y, :, c] if t == 0 else f.at[:, :, :, x, c]] * 2
        for n, region in enumerate(sent):
            remote(region, region, send_sem.at[t, n], recv_sem.at[t, 0, 0], index_of(z, y, x, 1 - c)).wait_send()
        for p in (0, 1):
            plane(p, t, False).wait_send()
        for j in (1, 2, 3):
            for way in (1, -1):
                @pl.when(within(z - way * (j - 1)) & within(z + way))
                def _():
                    line(j, t, way, False).wait_send()
    if save:
        for m in range(tiles):
            u_save(layers - 1, pl.ds(m * TILE, TILE), m).wait()
        h[...] = (h[...] - y_in[...].astype(F32)) / scale
        at_save(layers - 1).wait()
        zt_save(layers - 1).wait()


def forward(save, ident, w1f, w2f, x_in, y_in=None, scale=None):
    layers, r1, d_ff = w1f.shape
    r2 = w2f.shape[1]
    tok, d_model = x_in.shape
    tiles = tok // TILE
    sds = jax.ShapeDtypeStruct
    hbm, vmem = pl.BlockSpec(memory_space=pl.ANY), pl.BlockSpec(memory_space=pltpu.VMEM)
    outs = [sds((layers, 4, 2, 2, 2, r1, d_ff), BF16), sds((layers, 4, 2, 2, 2, r2, d_model), BF16), sds((tok, d_model), F32)]
    out_specs = [hbm, hbm, vmem]
    scratch = [
        pltpu.VMEM((layers, r1, d_ff), BF16),
        pltpu.VMEM((layers, r2, d_model), BF16),
        pltpu.VMEM((4, 2, 2, 2, r1, d_ff), BF16),
        pltpu.VMEM((4, 2, 2, 2, r2, d_model), BF16),
        pltpu.SemaphoreType.DMA((2,)),
        pltpu.SemaphoreType.DMA((2,)),
        pltpu.SemaphoreType.DMA((2, 9)),
        pltpu.SemaphoreType.DMA((2, layers, 8)),
        pltpu.SemaphoreType.DMA((2, 2, 6)),
    ]
    if save:
        outs += [sds((layers, tok, d_ff), F32), sds((layers, d_model, tok), BF16), sds((layers, d_ff, tok), BF16)]
        out_specs += [hbm, hbm, hbm]
        scratch += [
            pltpu.VMEM((tok, d_ff), F32),
            pltpu.VMEM((d_model, tok), BF16),
            pltpu.VMEM((d_ff, tok), BF16),
            pltpu.SemaphoreType.DMA((tiles + 2,)),
        ]
    return pl.pallas_call(
        functools.partial(forward_kernel, save, scale),
        out_shape=outs,
        in_specs=[vmem] * (4 if save else 3),
        out_specs=out_specs,
        scratch_shapes=scratch,
        compiler_params=pltpu.CompilerParams(collective_id=ident, has_side_effects=True, vmem_limit_bytes=VMEM_BYTES),
        name="forward_save" if save else "forward_last",
    )(w1f, w2f, x_in, *([y_in] if save else []))


def gelu_back(u, q):
    t = jnp.tanh(GELU_K * (u + GELU_C * (u * u * u)))
    slope = 0.5 * (1.0 + t) + (0.5 * GELU_K) * u * (1.0 - t * t) * (1.0 + (3.0 * GELU_C) * (u * u))
    return slope * q


def backward_kernel(*refs):
    g1, g2, u_in, at_in, zt_in, d_in, s1, s2, d, d_low, w1v, w2v, u_v, at_v, zt_v, r_v = refs[:16]
    bufs = (refs[16:24], refs[24:32])
    late = (refs[32:35], refs[35:38])
    load_sem, send_sem, recv_sem, free_sem = refs[38:]
    sums = (s1, s2)
    layers = s1.shape[0]
    z, y, x, c = place()
    tok = d.shape[0]
    tiles = tok // TILE

    greet(z, y, x, c)

    x_peer, y_peer, core_peer = index_of(z, y, 1 - x, c), index_of(z, 1 - y, x, c), index_of(z, y, x, 1 - c)

    def peer_of(t, s):
        if s == 0:
            return core_peer
        return y_peer if (t == 0) == (s == 1) else x_peer

    def exchange(t, s):
        grad, got0, part, got1, quart, got2, line, got3 = bufs[t]
        if s == 0:
            src, dst = grad.at[:, :, :, 1 - c], got0
        else:
            src, dst = (part.at[:, 1 - y] if t == 0 else part.at[:, :, 1 - x]), got1
        return remote(src, dst, send_sem.at[t, s], recv_sem.at[t, s], peer_of(t, s))

    def trade(t, k):
        if k == 0:
            src, dst = late[t][0], late[t][1]
        else:
            quart, got2 = bufs[t][4], bufs[t][5]
            to = ring_z(z, k)
            src, dst = quart.at[to, 1 - x if t == 0 else 1 - y], got2.at[to]
        return remote(src, dst, send_sem.at[t, 6 + k], recv_sem.at[t, 6 + k], peer_of(t, 2))

    def line_send(t, k):
        line, got3 = bufs[t][6], bufs[t][7]
        to = ring_z(z, k)
        return remote(line.at[to], got3.at[k - 1], send_sem.at[t, 2 + k], recv_sem.at[t, 2 + k], index_of(to, y, x, c))

    def give(l, sem, peer):
        @pl.when(l > 0)
        def _():
            pl.semaphore_signal(sem, inc=1, device_id=(peer,), device_id_type=MESH)

    def take(l, sem):
        @pl.when(l < layers - 1)
        def _():
            pl.semaphore_wait(sem, 1)

    def send(t, s, l):
        take(l, free_sem.at[t, s])
        exchange(t, s).start()

    def add(a, b):
        return (a.astype(F32) + b.astype(F32)).astype(BF16)

    def finish(t, l):
        line, got3 = bufs[t][6], bufs[t][7]
        for k in (1, 2, 3):
            line_send(t, k).wait_recv()
        late[t][2][l] += got3[0].astype(F32) + got3[1].astype(F32) + got3[2].astype(F32)
        for k in (1, 2, 3):
            line_send(t, k).wait_send()
            give(l, free_sem.at[t, 2 + k], index_of(ring_z(z, -k), y, x, c))

    def to_line(t, l):
        quart, got2, line = bufs[t][4:7]
        for k in (1, 2, 3):
            trade(t, k).wait_recv()
        mine = x if t == 0 else y
        for k in (1, 2, 3):
            to = ring_z(z, k)
            line[to] = add(quart[to, mine], got2[to])
        late[t][2][l] = quart[z, mine].astype(F32)
        for k in (1, 2, 3):
            trade(t, k).wait_send()
        give(l, free_sem.at[t, 2], peer_of(t, 2))
        for k in (1, 2, 3):
            take(l, free_sem.at[t, 2 + k])
            line_send(t, k).start()

    def to_quart(t, l):
        part, got1, quart = bufs[t][2:5]
        exchange(t, 1).wait_recv()

        def body(zz, carry):
            for j in (0, 1):
                own = part[zz, y, j] if t == 0 else part[zz, j, x]
                quart[zz, j] = add(own, got1[zz, j])
            return carry

        lax.fori_loop(0, 4, body, 0)
        exchange(t, 1).wait_send()
        give(l, free_sem.at[t, 1], peer_of(t, 1))
        take(l, free_sem.at[t, 2])
        for k in (1, 2, 3):
            trade(t, k).start()
        late[t][0][l] = quart[z, 1 - x if t == 0 else 1 - y]

    def to_part(t, l):
        grad, got0, part = bufs[t][:3]
        exchange(t, 0).wait_recv()

        def body(zz, carry):
            for yy in (0, 1):
                for xx in (0, 1):
                    part[zz, yy, xx] = add(grad[zz, yy, xx, c], got0[zz, yy, xx])
            return carry

        lax.fori_loop(0, 4, body, 0)
        exchange(t, 0).wait_send()
        give(l, free_sem.at[t, 0], peer_of(t, 0))
        send(t, 1, l)

    loads = (
        (lambda l: g1.at[l], w1v),
        (lambda l: g2.at[l], w2v),
        (lambda l: u_in.at[l], u_v),
        (lambda l: at_in.at[l], at_v),
        (lambda l: zt_in.at[l], zt_v),
    )

    def load(n, l):
        return pltpu.make_async_copy(loads[n][0](l), loads[n][1], load_sem.at[n])

    def prefetch(n, l):
        @pl.when(l > 0)
        def _():
            load(n, l - 1).start()

    def put(t, zz, res):
        grad = bufs[t][0]
        rows = grad.shape[4]
        for k in range(8):
            grad[zz, k // 4, k // 2 % 2, k % 2] = res[k * rows:(k + 1) * rows].astype(BF16)

    def compute(l):
        d_low[...] = d[...].astype(BF16)
        load(4, l).wait()

        def grad_two(zz, carry):
            step = d_two // 4
            put(1, zz, dot(zt_v[pl.ds(pl.multiple_of(zz * step, step), step), :], d_low[...]))
            return carry

        d_two = zt_v.shape[0]
        lax.fori_loop(0, 4, grad_two, 0)
        send(1, 0, l)
        prefetch(4, l)
        load(1, l).wait()
        load(2, l).wait()

        def pre(m, carry):
            rows = pl.ds(pl.multiple_of(m * TILE, TILE), TILE)
            q = dot_t(d_low[rows, :], whole(w2v))
            r_v[rows, :] = gelu_back(u_v[rows, :], q).astype(BF16)
            return carry

        lax.fori_loop(0, tiles, pre, 0)
        prefetch(1, l)
        prefetch(2, l)
        load(3, l).wait()

        def grad_one(zz, carry):
            step = at_v.shape[0] // 4
            put(0, zz, dot(at_v[pl.ds(pl.multiple_of(zz * step, step), step), :], r_v[...]))
            return carry

        lax.fori_loop(0, 4, grad_one, 0)
        send(0, 0, l)
        prefetch(3, l)
        load(0, l).wait()

        @pl.when(l > 0)
        def _():
            def back(m, carry):
                rows = pl.ds(pl.multiple_of(m * TILE, TILE), TILE)
                d[rows, :] += dot_t(r_v[rows, :], whole(w1v))
                return carry

            lax.fori_loop(0, tiles, back, 0)

        prefetch(0, l)

    first = pltpu.make_async_copy(d_in, d, load_sem.at[len(loads)])
    first.start()
    for n in range(len(loads)):
        load(n, layers - 1).start()
    first.wait()

    def step(it, carry):
        l = layers - 1 - it
        for lag, stage in ((4, finish), (3, to_line), (2, to_quart), (1, to_part)):
            @pl.when((l + lag >= 0) & (l + lag < layers))
            def _():
                for t in (1, 0):
                    stage(t, l + lag)

        @pl.when(l + 2 == 0)
        def _():
            for t in (0, 1):
                trade(t, 0).start()

        @pl.when(l >= 0)
        def _():
            compute(l)

        return carry

    lax.fori_loop(0, layers + 4, step, 0)

    for t in (0, 1):
        trade(t, 0).wait()

    def total(l, carry):
        for t in (0, 1):
            sums[t][l] = (late[t][2][l] + late[t][1][l].astype(F32)).astype(BF16)
        return carry

    lax.fori_loop(0, layers, total, 0)


def backward(ident, g1, g2, u_all, at_all, zt_all, d_state):
    layers, r1, d_ff = g1.shape[0], g1.shape[5], g1.shape[6]
    r2 = g2.shape[5]
    tok, d_model = d_state.shape
    sds = jax.ShapeDtypeStruct
    hbm, vmem = pl.BlockSpec(memory_space=pl.ANY), pl.BlockSpec(memory_space=pltpu.VMEM)
    scratch = [
        pltpu.VMEM((tok, d_model), F32),
        pltpu.VMEM((tok, d_model), BF16),
        pltpu.VMEM((4, 2, 2, 2, r1, d_ff), BF16),
        pltpu.VMEM((4, 2, 2, 2, r2, d_model), BF16),
        pltpu.VMEM((tok, d_ff), F32),
        pltpu.VMEM((d_model, tok), BF16),
        pltpu.VMEM((d_ff, tok), BF16),
        pltpu.VMEM((tok, d_ff), BF16),
    ]
    for block in ((r1, d_ff), (r2, d_model)):
        for lead in ((4, 2, 2, 2), (4, 2, 2), (4, 2, 2), (4, 2), (4, 2), (4,), (4,), (3,)):
            scratch.append(pltpu.VMEM(lead + block, BF16))
    for block in ((r1, d_ff), (r2, d_model)):
        scratch += [pltpu.VMEM((layers,) + block, kind) for kind in (BF16, BF16, F32)]
    scratch += [
        pltpu.SemaphoreType.DMA((6,)),
        pltpu.SemaphoreType.DMA((2, 10)),
        pltpu.SemaphoreType.DMA((2, 10)),
        pltpu.SemaphoreType.REGULAR((2, 6)),
    ]
    return pl.pallas_call(
        backward_kernel,
        out_shape=[sds((layers, r1, d_ff), BF16), sds((layers, r2, d_model), BF16)],
        in_specs=[hbm] * 6,
        out_specs=[vmem, vmem],
        scratch_shapes=scratch,
        compiler_params=pltpu.CompilerParams(collective_id=ident, has_side_effects=True, vmem_limit_bytes=VMEM_BYTES),
        name="backward",
    )(g1, g2, u_all, at_all, zt_all, d_state)


def solution(mesh):
    n_dev = mesh.shape["data"]
    w_spec = P(None, "data", None)
    row_spec = P("data", None)

    def device_step(w_one, w_two, mom_one, mom_two, x_zero, y_zero, x_one, y_one):
        tok_dev, d_model = x_zero.shape
        scale = n_dev * tok_dev * d_model
        g1, g2, d_state, u_all, at_all, zt_all = forward(True, 0, w_one, w_two, x_zero, y_zero, scale)
        sum_one, sum_two = backward(1, g1, g2, u_all, at_all, zt_all, d_state)
        new_mom_one = MOMENTUM * mom_one + sum_one.astype(F32)
        new_mom_two = MOMENTUM * mom_two + sum_two.astype(F32)
        new_w_one = w_one - LEARN_RATE * new_mom_one
        new_w_two = w_two - LEARN_RATE * new_mom_two
        h_last = forward(False, 2, new_w_one, new_w_two, x_one)[2]
        loss_rows = jnp.sum(jnp.square(h_last - y_one.astype(F32)), axis=1) / (2 * d_model)
        return new_w_one, new_w_two, new_mom_one, new_mom_two, loss_rows, h_last

    return jax.shard_map(device_step, mesh=mesh, in_specs=(w_spec, w_spec, w_spec, w_spec, row_spec, row_spec, row_spec, row_spec), out_specs=(w_spec, w_spec, w_spec, w_spec, P("data"), row_spec), check_vma=False)
```

```python
import functools
import math

import jax
import jax.numpy as jnp
from jax import lax
from jax.experimental import pallas as pl
from jax.experimental.pallas import tpu as pltpu
from jax.sharding import PartitionSpec as P

LEARN_RATE = 0.1
MOMENTUM = 0.9
MESH = pl.DeviceIdType.MESH
F32 = jnp.float32
BF16 = jnp.bfloat16
TILE = 256
AHEAD = 5
LINE_AT = 0
VMEM_BYTES = 67_000_000
GELU_K = math.sqrt(2.0 / math.pi)
GELU_C = 0.044715


def place():
    me = lax.axis_index("data")
    return lax.div(me, 8), lax.rem(lax.div(me, 4), 2), lax.rem(lax.div(me, 2), 2), lax.rem(me, 2)


def index_of(z, y, x, c):
    return ((z * 2 + y) * 2 + x) * 2 + c


def ring_z(z, step):
    return lax.rem(z + step + 4, 4)


def greet(z, y, x, c):
    barrier = pltpu.get_barrier_semaphore()
    peers = [index_of(ring_z(z, k), y, x, c) for k in (1, 2, 3)]
    peers += [index_of(z, y, 1 - x, c), index_of(z, 1 - y, x, c), index_of(z, y, x, 1 - c)]
    for peer in peers:
        pl.semaphore_signal(barrier, inc=1, device_id=(peer,), device_id_type=MESH)
    pl.semaphore_wait(barrier, len(peers))


def remote(src, dst, send_sem, recv_sem, peer):
    return pltpu.make_async_remote_copy(
        src_ref=src, dst_ref=dst, send_sem=send_sem, recv_sem=recv_sem, device_id=(peer,), device_id_type=MESH
    )


def dot(a, b):
    return jnp.dot(a, b, preferred_element_type=F32)


def dot_t(a, b):
    return lax.dot_general(a, b, (((1,), (1,)), ((), ())), preferred_element_type=F32)


def whole(blocks):
    w = blocks[...]
    return w.reshape(math.prod(w.shape[:-1]), w.shape[-1])


def gelu(u):
    return (0.5 * u) * (1.0 + jnp.tanh(GELU_K * (u + GELU_C * (u * u * u))))


def forward_kernel(save, scale, *refs):
    w1f, w2f, x_in, y_in = refs[:4] if save else refs[:3] + (None,)
    g1, g2, h = refs[4:7] if save else refs[3:6]
    refs = refs[7:] if save else refs[6:]
    if save:
        u_out, at_out, zt_out = refs[:3]
        refs = refs[3:]
    w1s, w2s = refs[:2]
    refs = refs[2:]
    far = 6 if save else 5
    w1v, w2v, own_sem, load_sem, send_sem, recv_sem, line_sems = refs[:7]
    if save:
        u_v, at_v, zt_v, save_sem = refs[7:]
    layers = w1s.shape[0]
    z, y, x, c = place()
    shard, full = (w1s, w2s), (g1, g2)
    tiles = x_in.shape[0] // TILE
    w1s[...] = w1f[...].astype(BF16)
    w2s[...] = w2f[...].astype(BF16)

    greet(z, y, x, c)

    def z_copy(t, l, k, from_z):
        return remote(
            shard[t].at[l], full[t].at[l, from_z, y, x, c], send_sem.at[t, k - 1], recv_sem.at[t, l, k - 1],
            index_of(ring_z(z, k), y, x, c),
        )

    def half(t, l, other, core):
        g = full[t].at[l]
        if t == 0:
            return g.at[:, 1 - y if other else y, :, core]
        return g.at[:, :, 1 - x if other else x, core]

    def hop(t, s, l, arriving):
        if s == 1:
            region = half(t, l, arriving, c)
            peer = index_of(z, 1 - y, x, c) if t == 0 else index_of(z, y, 1 - x, c)
        else:
            region = half(t, l, s == 3, 1 - c if arriving else c)
            peer = index_of(z, y, x, 1 - c)
        return remote(region, region, send_sem.at[t, 3 + s], recv_sem.at[t, l, 3 + s], peer)

    def first(t, l, k):
        region = full[t].at[l, ring_z(z, -k), y, x, c]
        src = region if k else shard[t].at[l]
        peer = index_of(z, y, 1 - x, c) if t == 0 else index_of(z, 1 - y, x, c)
        return remote(src, region, send_sem.at[t, 3], recv_sem.at[t, l, 3 if k else 7], peer)

    def first_arrived(t, l):
        first(t, l, 0).wait_recv()
        region = full[t].at[l, 0:3, y, x, c]
        remote(region, region, send_sem.at[t, 3], recv_sem.at[t, l, 3], index_of(z, y, x, 1 - c)).wait_recv()

    def plane(p, t, arriving):
        along_x = (t == 0) == (p == 0)
        xs = 1 - x if arriving and along_x else x
        ys = 1 - y if arriving and not along_x else y
        g = full[t].at[far, z]
        if p == 0:
            region = g.at[ys, xs, c]
        else:
            region = g.at[:, xs, c] if along_x else g.at[ys, :, c]
        src = region if p or arriving else shard[t].at[far]
        peer = index_of(z, y, 1 - x, c) if along_x else index_of(z, 1 - y, x, c)
        return remote(src, region, send_sem.at[t, 7 + p], recv_sem.at[t, far, p], peer)

    def line(j, t, way, arriving):
        region = full[t].at[far, z - way * (j if arriving else j - 1), :, :, c]
        n = 2 * j - 2 + (way > 0)
        return remote(region, region, line_sems.at[0, t, n], line_sems.at[1, t, n], index_of(z + way, y, x, c))

    def skip_far(n):
        return jnp.where(n < far, n, n + 1)

    def within(zz):
        return (zz >= 0) & (zz < 4)

    def line_step(j):
        for t in (0, 1):
            for way in (1, -1):
                if j > 1:
                    @pl.when(within(z - way * (j - 1)))
                    def _():
                        line(j - 1, t, way, True).wait_recv()
                if j < 4:
                    @pl.when(within(z - way * (j - 1)) & within(z + way))
                    def _():
                        line(j, t, way, False).start()

    def send_z(l, carry):
        @pl.when(l != far)
        def _():
            for t in (0, 1):
                for k in (1, 2, 3):
                    z_copy(t, l, k, z).start()
        return carry

    def send_own(l, carry):
        @pl.when(l != far)
        def _():
            for t in (0, 1):
                first(t, l, 0).start()
        return carry

    def z_to_first(t, l):
        for k in (1, 2, 3):
            z_copy(t, l, k, ring_z(z, -k)).wait_recv()
            first(t, l, k).start()

    def to_plane(t, l):
        first_arrived(t, l)
        hop(t, 1, l, False).start()
        hop(t, 2, l, False).start()

    def to_core(t, l):
        hop(t, 1, l, True).wait_recv()
        hop(t, 3, l, False).start()

    own = [pltpu.make_async_copy(shard[t], full[t].at[:, z, y, x, c], own_sem.at[t]) for t in (0, 1)]
    for t in (0, 1):
        plane(0, t, False).start()
    lax.fori_loop(0, AHEAD, send_z, 0)
    lax.fori_loop(0, layers, send_own, 0)
    for copy in own:
        copy.start()
    h[...] = x_in[...].astype(F32)
    for t in (0, 1):
        own[t].wait()
        plane(0, t, True).wait_recv()
        plane(1, t, False).start()

    def u_save(l, rows, m):
        return pltpu.make_async_copy(u_v.at[rows], u_out.at[l, rows], save_sem.at[m])

    def at_save(l):
        return pltpu.make_async_copy(at_v, at_out.at[l], save_sem.at[tiles])

    def zt_save(l):
        return pltpu.make_async_copy(zt_v, zt_out.at[l], save_sem.at[tiles + 1])

    def load(t, l, n):
        core = 1 - c if n else c
        return pltpu.make_async_copy(
            full[t].at[l, :, :, :, core], (w1v, w2v)[t].at[:, :, :, core], load_sem.at[t, n]
        )

    def compute(l):
        if save:
            @pl.when(l > 0)
            def _():
                at_save(l - 1).wait()
                zt_save(l - 1).wait()
        for n in (0, 1):
            load(0, l, n).wait()

        def tile(m, carry):
            start = pl.multiple_of(m * TILE, TILE)
            rows = pl.ds(start, TILE)
            a = h[rows, :].astype(BF16)
            u = dot(a, whole(w1v))
            act = gelu(u).astype(BF16)

            @pl.when(m == 0)
            def _():
                for n in (0, 1):
                    load(1, l, n).wait()

            if save:
                @pl.when(l > 0)
                def _():
                    u_save(l - 1, rows, m).wait()
                u_v[rows, :] = u
                u_save(l, rows, m).start()
                at_v[:, rows] = a.T
                zt_v[:, rows] = act.T
            h[rows, :] += dot(act, whole(w2v))
            return carry

        lax.fori_loop(0, tiles, tile, 0)
        if save:
            at_save(l).start()
            zt_save(l).start()

    for stage in (z_to_first, to_plane):
        for t in (0, 1):
            stage(t, 0)
    for l in (1, 2):
        for t in (0, 1):
            z_to_first(t, l)
    for t in (0, 1):
        to_plane(t, 1)
    for t in (0, 1):
        to_core(t, 0)

    def step(l, carry):
        for t in (0, 1):
            load(t, l, 0).start()

        @pl.when(l + AHEAD < layers)
        def _():
            send_z(l + AHEAD, 0)

        third, second = skip_far(l + 3), skip_far(l + 2)

        @pl.when(third < layers)
        def _():
            for t in (0, 1):
                z_to_first(t, third)

        @pl.when(second < layers)
        def _():
            for t in (0, 1):
                to_plane(t, second)

        for j in (1, 2, 3, 4):
            @pl.when(l == LINE_AT + j)
            def _():
                if j == 1:
                    for t in (0, 1):
                        plane(1, t, True).wait_recv()
                line_step(j)

        for t in (0, 1):
            hop(t, 2, l, True).wait_recv()
            hop(t, 3, l, True).wait_recv()
            load(t, l, 1).start()
        compute(l)

        @pl.when(l + 1 < layers)
        def _():
            for t in (0, 1):
                @pl.when(l + 1 != far)
                def _():
                    to_core(t, l + 1)

                @pl.when(l + 1 == far)
                def _():
                    hop(t, 2, far, False).start()
                    hop(t, 3, far, False).start()

        return carry

    lax.fori_loop(0, layers, step, 0)

    others = pl.ds(0, layers - 1)
    for t in (0, 1):
        f = full[t]
        sent = [f.at[others, z, y, x, c]] * 3
        sent += [f.at[others, :, y, x, c], f.at[others, :, y, :, c] if t == 0 else f.at[others, :, :, x, c]]
        sent += [f.at[:, :, y, :, c] if t == 0 else f.at[:, :, :, x, c]] * 2
        for n, region in enumerate(sent):
            remote(region, region, send_sem.at[t, n], recv_sem.at[t, 0, 0], index_of(z, y, x, 1 - c)).wait_send()
        for p in (0, 1):
            plane(p, t, False).wait_send()
        for j in (1, 2, 3):
            for way in (1, -1):
                @pl.when(within(z - way * (j - 1)) & within(z + way))
                def _():
                    line(j, t, way, False).wait_send()
    if save:
        for m in range(tiles):
            u_save(layers - 1, pl.ds(m * TILE, TILE), m).wait()
        h[...] = (h[...] - y_in[...].astype(F32)) / scale
        at_save(layers - 1).wait()
        zt_save(layers - 1).wait()


def forward(save, ident, w1f, w2f, x_in, y_in=None, scale=None):
    layers, r1, d_ff = w1f.shape
    r2 = w2f.shape[1]
    tok, d_model = x_in.shape
    tiles = tok // TILE
    sds = jax.ShapeDtypeStruct
    hbm, vmem = pl.BlockSpec(memory_space=pl.ANY), pl.BlockSpec(memory_space=pltpu.VMEM)
    outs = [sds((layers, 4, 2, 2, 2, r1, d_ff), BF16), sds((layers, 4, 2, 2, 2, r2, d_model), BF16), sds((tok, d_model), F32)]
    out_specs = [hbm, hbm, vmem]
    scratch = [
        pltpu.VMEM((layers, r1, d_ff), BF16),
        pltpu.VMEM((layers, r2, d_model), BF16),
        pltpu.VMEM((4, 2, 2, 2, r1, d_ff), BF16),
        pltpu.VMEM((4, 2, 2, 2, r2, d_model), BF16),
        pltpu.SemaphoreType.DMA((2,)),
        pltpu.SemaphoreType.DMA((2, 2)),
        pltpu.SemaphoreType.DMA((2, 9)),
        pltpu.SemaphoreType.DMA((2, layers, 8)),
        pltpu.SemaphoreType.DMA((2, 2, 6)),
    ]
    if save:
        outs += [sds((layers, tok, d_ff), F32), sds((layers, d_model, tok), BF16), sds((layers, d_ff, tok), BF16)]
        out_specs += [hbm, hbm, hbm]
        scratch += [
            pltpu.VMEM((tok, d_ff), F32),
            pltpu.VMEM((d_model, tok), BF16),
            pltpu.VMEM((d_ff, tok), BF16),
            pltpu.SemaphoreType.DMA((tiles + 2,)),
        ]
    return pl.pallas_call(
        functools.partial(forward_kernel, save, scale),
        out_shape=outs,
        in_specs=[vmem] * (4 if save else 3),
        out_specs=out_specs,
        scratch_shapes=scratch,
        compiler_params=pltpu.CompilerParams(collective_id=ident, has_side_effects=True, vmem_limit_bytes=VMEM_BYTES),
        name="forward_save" if save else "forward_last",
    )(w1f, w2f, x_in, *([y_in] if save else []))


def gelu_back(u, q):
    t = jnp.tanh(GELU_K * (u + GELU_C * (u * u * u)))
    slope = 0.5 * (1.0 + t) + (0.5 * GELU_K) * u * (1.0 - t * t) * (1.0 + (3.0 * GELU_C) * (u * u))
    return slope * q


def backward_kernel(*refs):
    g1, g2, u_in, at_in, zt_in, d_in, s1, s2, d, d_low, w1v, w2v, u_v, at_v, zt_v, r_v = refs[:16]
    bufs = (refs[16:24], refs[24:32])
    late = (refs[32:35], refs[35:38])
    load_sem, send_sem, recv_sem, free_sem = refs[38:]
    sums = (s1, s2)
    layers = s1.shape[0]
    z, y, x, c = place()
    tok = d.shape[0]
    tiles = tok // TILE

    greet(z, y, x, c)

    x_peer, y_peer, core_peer = index_of(z, y, 1 - x, c), index_of(z, 1 - y, x, c), index_of(z, y, x, 1 - c)

    def peer_of(t, s):
        if s == 0:
            return core_peer
        return y_peer if (t == 0) == (s == 1) else x_peer

    def exchange(t, s):
        grad, got0, part, got1, quart, got2, line, got3 = bufs[t]
        if s == 0:
            src, dst = grad.at[:, :, :, 1 - c], got0
        else:
            src, dst = (part.at[:, 1 - y] if t == 0 else part.at[:, :, 1 - x]), got1
        return remote(src, dst, send_sem.at[t, s], recv_sem.at[t, s], peer_of(t, s))

    def trade(t, k):
        if k == 0:
            src, dst = late[t][0], late[t][1]
        else:
            quart, got2 = bufs[t][4], bufs[t][5]
            to = ring_z(z, k)
            src, dst = quart.at[to, 1 - x if t == 0 else 1 - y], got2.at[to]
        return remote(src, dst, send_sem.at[t, 6 + k], recv_sem.at[t, 6 + k], peer_of(t, 2))

    def line_send(t, k):
        line, got3 = bufs[t][6], bufs[t][7]
        to = ring_z(z, k)
        return remote(line.at[to], got3.at[k - 1], send_sem.at[t, 2 + k], recv_sem.at[t, 2 + k], index_of(to, y, x, c))

    def give(l, sem, peer):
        @pl.when(l > 0)
        def _():
            pl.semaphore_signal(sem, inc=1, device_id=(peer,), device_id_type=MESH)

    def take(l, sem):
        @pl.when(l < layers - 1)
        def _():
            pl.semaphore_wait(sem, 1)

    def send(t, s, l):
        take(l, free_sem.at[t, s])
        exchange(t, s).start()

    def add(a, b):
        return (a.astype(F32) + b.astype(F32)).astype(BF16)

    def finish(t, l):
        line, got3 = bufs[t][6], bufs[t][7]
        for k in (1, 2, 3):
            line_send(t, k).wait_recv()
        late[t][2][l] += got3[0].astype(F32) + got3[1].astype(F32) + got3[2].astype(F32)
        for k in (1, 2, 3):
            line_send(t, k).wait_send()
            give(l, free_sem.at[t, 2 + k], index_of(ring_z(z, -k), y, x, c))

    def to_line(t, l):
        quart, got2, line = bufs[t][4:7]
        for k in (1, 2, 3):
            trade(t, k).wait_recv()
        mine = x if t == 0 else y
        for k in (1, 2, 3):
            to = ring_z(z, k)
            line[to] = add(quart[to, mine], got2[to])
        late[t][2][l] = quart[z, mine].astype(F32)
        for k in (1, 2, 3):
            trade(t, k).wait_send()
        give(l, free_sem.at[t, 2], peer_of(t, 2))
        for k in (1, 2, 3):
            take(l, free_sem.at[t, 2 + k])
            line_send(t, k).start()

    def to_quart(t, l):
        part, got1, quart = bufs[t][2:5]
        exchange(t, 1).wait_recv()

        def body(zz, carry):
            for j in (0, 1):
                own = part[zz, y, j] if t == 0 else part[zz, j, x]
                quart[zz, j] = add(own, got1[zz, j])
            return carry

        lax.fori_loop(0, 4, body, 0)
        exchange(t, 1).wait_send()
        give(l, free_sem.at[t, 1], peer_of(t, 1))
        take(l, free_sem.at[t, 2])
        for k in (1, 2, 3):
            trade(t, k).start()
        late[t][0][l] = quart[z, 1 - x if t == 0 else 1 - y]

    def to_part(t, l):
        grad, got0, part = bufs[t][:3]
        exchange(t, 0).wait_recv()

        def body(zz, carry):
            for yy in (0, 1):
                for xx in (0, 1):
                    part[zz, yy, xx] = add(grad[zz, yy, xx, c], got0[zz, yy, xx])
            return carry

        lax.fori_loop(0, 4, body, 0)
        exchange(t, 0).wait_send()
        give(l, free_sem.at[t, 0], peer_of(t, 0))
        send(t, 1, l)

    loads = (
        (lambda l: g1.at[l], w1v),
        (lambda l: g2.at[l], w2v),
        (lambda l: u_in.at[l], u_v),
        (lambda l: at_in.at[l], at_v),
        (lambda l: zt_in.at[l], zt_v),
    )

    def load(n, l):
        return pltpu.make_async_copy(loads[n][0](l), loads[n][1], load_sem.at[n])

    def prefetch(n, l):
        @pl.when(l > 0)
        def _():
            load(n, l - 1).start()

    def put(t, zz, res):
        grad = bufs[t][0]
        rows = grad.shape[4]
        for k in range(8):
            grad[zz, k // 4, k // 2 % 2, k % 2] = res[k * rows:(k + 1) * rows].astype(BF16)

    def compute(l):
        d_low[...] = d[...].astype(BF16)
        load(4, l).wait()

        def grad_two(zz, carry):
            step = d_two // 4
            put(1, zz, dot(zt_v[pl.ds(pl.multiple_of(zz * step, step), step), :], d_low[...]))
            return carry

        d_two = zt_v.shape[0]
        lax.fori_loop(0, 4, grad_two, 0)
        send(1, 0, l)
        prefetch(4, l)
        load(1, l).wait()
        load(2, l).wait()

        def pre(m, carry):
            rows = pl.ds(pl.multiple_of(m * TILE, TILE), TILE)
            q = dot_t(d_low[rows, :], whole(w2v))
            r_v[rows, :] = gelu_back(u_v[rows, :], q).astype(BF16)
            return carry

        lax.fori_loop(0, tiles, pre, 0)
        prefetch(1, l)
        prefetch(2, l)
        load(3, l).wait()

        def grad_one(zz, carry):
            step = at_v.shape[0] // 4
            put(0, zz, dot(at_v[pl.ds(pl.multiple_of(zz * step, step), step), :], r_v[...]))
            return carry

        lax.fori_loop(0, 4, grad_one, 0)
        send(0, 0, l)
        prefetch(3, l)
        load(0, l).wait()

        @pl.when(l > 0)
        def _():
            def back(m, carry):
                rows = pl.ds(pl.multiple_of(m * TILE, TILE), TILE)
                d[rows, :] += dot_t(r_v[rows, :], whole(w1v))
                return carry

            lax.fori_loop(0, tiles, back, 0)

        prefetch(0, l)

    first = pltpu.make_async_copy(d_in, d, load_sem.at[len(loads)])
    first.start()
    for n in range(len(loads)):
        load(n, layers - 1).start()
    first.wait()

    def step(it, carry):
        l = layers - 1 - it
        for lag, stage in ((4, finish), (3, to_line), (2, to_quart), (1, to_part)):
            @pl.when((l + lag >= 0) & (l + lag < layers))
            def _():
                for t in (1, 0):
                    stage(t, l + lag)

        @pl.when(l + 2 == 0)
        def _():
            for t in (0, 1):
                trade(t, 0).start()

        @pl.when(l >= 0)
        def _():
            compute(l)

        return carry

    lax.fori_loop(0, layers + 4, step, 0)

    for t in (0, 1):
        trade(t, 0).wait()

    def total(l, carry):
        for t in (0, 1):
            sums[t][l] = (late[t][2][l] + late[t][1][l].astype(F32)).astype(BF16)
        return carry

    lax.fori_loop(0, layers, total, 0)


def backward(ident, g1, g2, u_all, at_all, zt_all, d_state):
    layers, r1, d_ff = g1.shape[0], g1.shape[5], g1.shape[6]
    r2 = g2.shape[5]
    tok, d_model = d_state.shape
    sds = jax.ShapeDtypeStruct
    hbm, vmem = pl.BlockSpec(memory_space=pl.ANY), pl.BlockSpec(memory_space=pltpu.VMEM)
    scratch = [
        pltpu.VMEM((tok, d_model), F32),
        pltpu.VMEM((tok, d_model), BF16),
        pltpu.VMEM((4, 2, 2, 2, r1, d_ff), BF16),
        pltpu.VMEM((4, 2, 2, 2, r2, d_model), BF16),
        pltpu.VMEM((tok, d_ff), F32),
        pltpu.VMEM((d_model, tok), BF16),
        pltpu.VMEM((d_ff, tok), BF16),
        pltpu.VMEM((tok, d_ff), BF16),
    ]
    for block in ((r1, d_ff), (r2, d_model)):
        for lead in ((4, 2, 2, 2), (4, 2, 2), (4, 2, 2), (4, 2), (4, 2), (4,), (4,), (3,)):
            scratch.append(pltpu.VMEM(lead + block, BF16))
    for block in ((r1, d_ff), (r2, d_model)):
        scratch += [pltpu.VMEM((layers,) + block, kind) for kind in (BF16, BF16, F32)]
    scratch += [
        pltpu.SemaphoreType.DMA((6,)),
        pltpu.SemaphoreType.DMA((2, 10)),
        pltpu.SemaphoreType.DMA((2, 10)),
        pltpu.SemaphoreType.REGULAR((2, 6)),
    ]
    return pl.pallas_call(
        backward_kernel,
        out_shape=[sds((layers, r1, d_ff), BF16), sds((layers, r2, d_model), BF16)],
        in_specs=[hbm] * 6,
        out_specs=[vmem, vmem],
        scratch_shapes=scratch,
        compiler_params=pltpu.CompilerParams(collective_id=ident, has_side_effects=True, vmem_limit_bytes=VMEM_BYTES),
        name="backward",
    )(g1, g2, u_all, at_all, zt_all, d_state)


def solution(mesh):
    n_dev = mesh.shape["data"]
    w_spec = P(None, "data", None)
    row_spec = P("data", None)

    def device_step(w_one, w_two, mom_one, mom_two, x_zero, y_zero, x_one, y_one):
        tok_dev, d_model = x_zero.shape
        scale = n_dev * tok_dev * d_model
        g1, g2, d_state, u_all, at_all, zt_all = forward(True, 0, w_one, w_two, x_zero, y_zero, scale)
        sum_one, sum_two = backward(1, g1, g2, u_all, at_all, zt_all, d_state)
        new_mom_one = MOMENTUM * mom_one + sum_one.astype(F32)
        new_mom_two = MOMENTUM * mom_two + sum_two.astype(F32)
        new_w_one = w_one - LEARN_RATE * new_mom_one
        new_w_two = w_two - LEARN_RATE * new_mom_two
        h_last = forward(False, 2, new_w_one, new_w_two, x_one)[2]
        loss_rows = jnp.sum(jnp.square(h_last - y_one.astype(F32)), axis=1) / (2 * d_model)
        return new_w_one, new_w_two, new_mom_one, new_mom_two, loss_rows, h_last

    return jax.shard_map(device_step, mesh=mesh, in_specs=(w_spec, w_spec, w_spec, w_spec, row_spec, row_spec, row_spec, row_spec), out_specs=(w_spec, w_spec, w_spec, w_spec, P("data"), row_spec), check_vma=False)
```
